32 devices in a mesh: band: 8 (over y, x, core), chan: 4 (over z).
Axes of the slice: x: 2, y: 2, z: 4, core: 2. Of those that a mesh axis runs over, the one named last changes fastest.
Arguments:
- grid_feat: bfloat16 [2048, 468], P('band'), may hold values from -6 to 6
- w_embed: bfloat16 [468, 384], replicated, may hold values from -0.25 to 0.25
- w_send: bfloat16 [384, 384], P(None, 'chan'), may hold values from -0.3125 to 0.3125
- w_recv: bfloat16 [384, 384], P(None, 'chan'), may hold values from -0.3125 to 0.3125
- mesh_nodes: bfloat16 [2048, 384], P('band'), may hold values from -6 to 6
- mesh_cot: bfloat16 [2048, 384], P('band', 'chan'), may hold values from -0.049804688 to 0.049804688
- send_index: int32 [8, 2, 64], P('band'), may hold values from -1 to 255, as said below
- edge_source: int32 [32768], P('band'), may hold values from 0 to 383, as said below
- edge_receiver: int32 [32768], P('band'), may hold values from 0 to 255
Outputs:
- mesh_out: bfloat16 [2048, 384], P('band', 'chan')
- grad_embed: float32 [468, 384], P(None, 'chan')
- grad_send: float32 [384, 384], P(None, 'chan')
- grad_recv: float32 [384, 384], P(None, 'chan')
The draws below stay inside these ranges and needn't reach their ends.
Inputs may be any that keep to these rules, and one draw needn't show every extreme that they name: `send_index`: A block's first c slots hold rows (c from 32 to 64) and the rest hold -1; block [0, 0] and block [8 - 1, 1] hold only -1; for every band s one of its two blocks that are not all -1 has all 64 slots used (block [0, 1] for band 0, block [8 - 1, 0] for band 8 - 1). `edge_source`: every edge names a used slot of its partition, and every used slot is named by some edge of its partition.
All inputs are finite; a program needn't handle non-finite values.
Results may differ from the reference program's by a relative error of at most 0.011.
Values may be sent and summed in bfloat16 or wider, within the bound.
A program may use at most 64 MiB of HBM per device.

```python
import jax
import jax.numpy as jnp
from jax import lax

F = 468
L = 384
H = 384
G_DEV = 256
E_DEV = 4096
M_DEV = 256
CAP = 64
GRID = 2048
EDGES = 32768
MESH = 2048
N_BAND = 8


def count_table(key):
    lowest = max(2, CAP // 2)
    counts = jax.random.randint(jax.random.fold_in(key, 11), (N_BAND, 2), lowest, CAP + 1)
    full_side = jax.random.randint(jax.random.fold_in(key, 12), (N_BAND,), 0, 2)
    band = jnp.arange(N_BAND, dtype=jnp.int32)
    full_side = jnp.where(band == 0, 1, jnp.where(band == N_BAND - 1, 0, full_side))
    side = jnp.arange(2, dtype=jnp.int32)[None, :]
    counts = jnp.where(side == full_side[:, None], CAP, counts)
    exists = (side == 1) & (band[:, None] < N_BAND - 1) | (side == 0) & (band[:, None] > 0)
    return jnp.where(exists, counts, 0).astype(jnp.int32)


def draw_send_index(key, part):
    counts = count_table(key)
    grid_rows = jax.random.randint(jax.random.fold_in(key, 13), (N_BAND, 2, CAP), 0, G_DEV)
    slot_pos = jnp.arange(CAP, dtype=jnp.int32)[None, None, :]
    return jnp.where(slot_pos < counts[:, :, None], grid_rows, -1).astype(jnp.int32)


def draw_edge_source(key, part):
    counts = count_table(key)
    nothing = jnp.zeros((1,), dtype=jnp.int32)
    below = jnp.concatenate([nothing, counts[:-1, 1]])[:, None]
    above = jnp.concatenate([counts[1:, 0], nothing])[:, None]
    slot_width = G_DEV + 2 * CAP
    position = jnp.arange(E_DEV, dtype=jnp.int32)[None, :]
    valid_total = G_DEV + below + above
    drawn = jax.random.randint(jax.random.fold_in(key, 14), (N_BAND, E_DEV), 0, valid_total)
    placed = jnp.where(drawn < G_DEV + below, drawn, drawn - below + CAP)
    valid = (position < G_DEV) | (position >= G_DEV) & (position < G_DEV + below) | (position >= G_DEV + CAP) & (position < G_DEV + CAP + above)
    leading = jnp.where(valid, position, position % G_DEV)
    ordered = jnp.where(position < slot_width, leading, placed).astype(jnp.int32)
    row_keys = jax.random.split(jax.random.fold_in(key, 16), N_BAND)
    orders = jax.vmap(lambda one_key: jax.random.permutation(one_key, E_DEV))(row_keys)
    shuffled = jnp.take_along_axis(ordered, orders.astype(jnp.int32), axis=1)
    return shuffled.reshape(-1).astype(jnp.int32)


def place_ends(result, rng, smallest, high):
    index_at = [jax.random.randint(jax.random.fold_in(rng, axis), (), 0, length) for axis, length in enumerate(result.shape)]
    longest = result.shape.index(max(result.shape))
    neighbour = index_at[:longest] + [(index_at[longest] + 1) % result.shape[longest]] + index_at[longest + 1:]
    return result.at[tuple(index_at)].set(smallest).at[tuple(neighbour)].set(high)


def shard_levels(stream_key, shape, pieces, smallest, largest):
    def one(axis_at, shards_of):
        draws = jax.random.uniform(jax.random.fold_in(jax.random.fold_in(stream_key, 6), axis_at), (shards_of,), jnp.float32, smallest / len(pieces), largest / len(pieces))
        return jnp.repeat(jnp.exp(draws), shape[axis_at] // shards_of).reshape((-1,) + (1,) * (len(shape) - axis_at - 1))

    factor_of = one(*pieces[0])
    for cut in pieces[1:]:
        factor_of = factor_of * one(*cut)
    return factor_of


def scatter_about(stream_key, extent, spread, most, shards=(), held_as=jnp.bfloat16):
    result = spread * jax.random.normal(stream_key, extent, jnp.float32)
    if shards:
        result = result * shard_levels(stream_key, extent, shards, -0.22, 0.18)
    return jnp.clip(result, -most, most).astype(held_as)


def setup_inputs(seed: int = 0) -> dict:
    seeds = jax.random.split(jax.random.key(seed), 10)
    return {
        "grid_feat": scatter_about(seeds[0], (GRID, F), 1.0, 6.0, ((0, 8),)),
        "w_embed": scatter_about(seeds[1], (F, L), F ** -0.5, 0.25),
        "w_send": scatter_about(seeds[2], (L, H), L ** -0.5, 0.3125, ((1, 4),)),
        "w_recv": scatter_about(seeds[3], (L, H), L ** -0.5, 0.3125, ((1, 4),)),
        "mesh_nodes": scatter_about(seeds[4], (MESH, L), 1.0, 6.0, ((0, 8),)),
        "mesh_cot": scatter_about(seeds[5], (MESH, H), 0.008, 0.049804688, ((0, 8), (1, 4))),
        "send_index": draw_send_index(jax.random.fold_in(seeds[9], 71), 0),
        "edge_source": draw_edge_source(jax.random.fold_in(seeds[9], 71), 0),
        "edge_receiver": place_ends(jax.random.randint(seeds[8], (EDGES,), 0, M_DEV), jax.random.fold_in(seeds[8], 1), 0, M_DEV - 1).astype(jnp.int32),
    }


def silu_slope(inputs):
    sigmoid_v = jax.nn.sigmoid(inputs)
    return sigmoid_v * (1.0 + inputs * (1.0 - sigmoid_v))


def reference(grid_feat, w_embed, w_send, w_recv, mesh_nodes, mesh_cot, send_index, edge_source, edge_receiver):
    grid_pre = jnp.dot(grid_feat, w_embed, preferred_element_type=jnp.float32)
    latent = jax.nn.silu(grid_pre).astype(jnp.bfloat16)
    slot_width = G_DEV + 2 * CAP
    blank = jnp.full((1, 2, CAP), -1, dtype=jnp.int32)
    padded_index = jnp.concatenate([blank, send_index.astype(jnp.int32), blank], axis=0)
    below = padded_index[0:N_BAND, 1]
    above = padded_index[2:N_BAND + 2, 0]
    bands = jnp.arange(N_BAND, dtype=jnp.int32)[:, None]
    own_ids = bands * G_DEV + jnp.arange(G_DEV, dtype=jnp.int32)[None, :]
    below_ids = jnp.where(below >= 0, (bands - 1) * G_DEV + below, GRID)
    above_ids = jnp.where(above >= 0, (bands + 1) * G_DEV + above, GRID)
    slot_node = jnp.concatenate([own_ids, below_ids, above_ids], axis=1).astype(jnp.int32)

    def partition(items):
        node_ids, sources, receivers, nodes, cotan = items
        rows = latent[jnp.minimum(node_ids, GRID - 1)]
        send_proj = jnp.dot(rows, w_send, preferred_element_type=jnp.float32)
        recv_proj = jnp.dot(nodes, w_recv, preferred_element_type=jnp.float32)
        edge_pre = send_proj[sources] + recv_proj[receivers]
        message = jax.nn.silu(edge_pre).astype(jnp.bfloat16)
        out_block = jax.ops.segment_sum(message.astype(jnp.float32), receivers, M_DEV).astype(jnp.bfloat16)
        edge_grad = (cotan[receivers].astype(jnp.float32) * silu_slope(edge_pre)).astype(jnp.bfloat16)
        slot_grad = jax.ops.segment_sum(edge_grad.astype(jnp.float32), sources, slot_width).astype(jnp.bfloat16)
        recv_grad = jax.ops.segment_sum(edge_grad.astype(jnp.float32), receivers, M_DEV).astype(jnp.bfloat16)
        send_part = jnp.dot(rows.T, slot_grad, preferred_element_type=jnp.float32)
        recv_part = jnp.dot(nodes.T, recv_grad, preferred_element_type=jnp.float32)
        slot_back = jnp.dot(slot_grad, w_send.T, preferred_element_type=jnp.float32)
        return out_block, send_part, recv_part, slot_back

    out_blocks, send_parts, recv_parts, slot_backs = lax.map(partition, (
        slot_node,
        edge_source.reshape(N_BAND, E_DEV).astype(jnp.int32),
        edge_receiver.reshape(N_BAND, E_DEV).astype(jnp.int32),
        mesh_nodes.reshape(N_BAND, M_DEV, L),
        mesh_cot.reshape(N_BAND, M_DEV, H)))
    mesh_out = out_blocks.reshape(MESH, H)
    grad_send = jnp.sum(send_parts, axis=0)
    grad_recv = jnp.sum(recv_parts, axis=0)
    grid_grad = jax.ops.segment_sum(slot_backs.reshape(-1, L), slot_node.reshape(-1), GRID)
    pre_grad = (grid_grad * silu_slope(grid_pre)).astype(jnp.bfloat16)
    grad_embed = jnp.dot(grid_feat.T, pre_grad, preferred_element_type=jnp.float32)
    return mesh_out, grad_embed, grad_send, grad_recv
```

```python
import functools
import math

import jax
import jax.numpy as jnp
from jax import lax
from jax.experimental import pallas as pl
from jax.experimental.pallas import tpu as pltpu
from jax.sharding import PartitionSpec as P

BF = jnp.bfloat16
F32 = jnp.float32
MESH = pl.DeviceIdType.MESH
LANES = 128


def mm(a, b):
    return lax.dot_general(a, b, (((1,), (0,)), ((), ())), preferred_element_type=F32)


def mm_tn(a, b):
    return lax.dot_general(a, b, (((0,), (0,)), ((), ())), preferred_element_type=F32)


def mm_nt(a, b):
    return lax.dot_general(a, b, (((1,), (1,)), ((), ())), preferred_element_type=F32)


def eye(size):
    row = lax.broadcasted_iota(jnp.int32, (size, size), 0)
    col = lax.broadcasted_iota(jnp.int32, (size, size), 1)
    return jnp.where(row == col, 1.0, 0.0).astype(BF)


def sigmoid(v):
    return 0.5 + 0.5 * jnp.tanh(0.5 * v)


def body(
    bands, chans, chunk,
    feat_in, embed_in, wsend_in, wrecv_in, nodes_in, cot_in, send_in, source_in, receiver_in,
    mesh_out, late_out, send_out, recv_out,
    feat, embed, wsend, wrecv, nodes, cot, send, source, receiver, loads,
    latent, slope, outgoing, outer, feat_out, feat_rows, latent_rows, slope_rows,
    tables, hot_recv, hot_src, drawn, pairs, acc, total,
    part_own, part_out, part_in, z_out, z_in, planes, final,
    e_own, e_out, e_in, e_planes, e_final,
    row_send, row_recv, feat_send, feat_recv, part_send, part_recv, z_send, z_recv,
    plane_send, plane_recv, final_send, final_recv, e_send, e_recv, ep_send, ep_recv, ef_send, ef_recv,
):
    band = lax.axis_index("band")
    chan = lax.axis_index("chan")
    chips = bands // 2
    core = lax.rem(band, 2)
    chip = lax.div(band, 2)
    width = wsend.shape[0]
    grid = feat.shape[1]
    inputs = feat.shape[0]
    latents = embed.shape[1]
    mesh_count = nodes.shape[0]
    cap = outgoing.shape[0] // 2
    slots = grid + 2 * cap
    steps = source.shape[0] // chunk
    cuts = [(at, min(at + LANES, inputs)) for at in range(0, inputs, LANES)]
    left = lax.rem(band + bands - 1, bands)
    right = lax.rem(band + 1, bands)
    mate = band + 1 - 2 * core
    peers = [2 * lax.rem(chip + step, chips) + core for step in range(1, chips)]
    others = [lax.rem(chan + step, chans) for step in range(1, chans)]

    barrier = pltpu.get_barrier_semaphore()
    for peer in [left, right, mate] + peers:
        pl.semaphore_signal(barrier, inc=1, device_id=(peer, chan), device_id_type=MESH)
    for peer in others:
        pl.semaphore_signal(barrier, inc=1, device_id=(band, peer), device_id_type=MESH)

    pulls = {}
    for at, (name, src, dst) in enumerate(
        (
            ("send", send_in, send), ("feat", feat_in, feat), ("embed", embed_in, embed),
            ("wsend", wsend_in, wsend), ("nodes", nodes_in, nodes), ("wrecv", wrecv_in, wrecv),
            ("cot", cot_in, cot), ("source", source_in, source), ("receiver", receiver_in, receiver),
        )
    ):
        pulls[name] = pltpu.make_async_copy(src, dst, loads.at[at])
        pulls[name].start()

    def remote(src, dst, send_sem, recv_sem, to_band, to_chan):
        return pltpu.make_async_remote_copy(
            src_ref=src, dst_ref=dst, send_sem=send_sem, recv_sem=recv_sem,
            device_id=(to_band, to_chan), device_id_type=MESH,
        )

    pulls["send"].wait()
    picks = lax.broadcasted_iota(jnp.int32, (grid, 2 * cap), 0) == jnp.concatenate(
        [send[0, 0:1, :], send[0, 1:2, :]], axis=1
    )
    pick_rows = jnp.transpose(jnp.where(picks, 1.0, 0.0)).astype(BF)
    pulls["feat"].wait()
    pulls["embed"].wait()
    pre = mm_tn(embed[...], feat[...])
    gate = sigmoid(pre)
    silu = pre * gate
    latent[...] = silu.astype(BF)
    slope[...] = gate + silu * (1.0 - gate)
    pulls["wsend"].wait()
    own = mm(wsend[...], latent[...]).astype(BF)
    outgoing[...] = mm_nt(pick_rows, own).astype(BF)
    if inputs < feat_out.shape[1]:
        feat_out[...] = jnp.zeros_like(feat_out)
    feat_out[:, :inputs] = mm_nt(pick_rows, feat[...]).astype(BF)
    pl.semaphore_wait(barrier, 3 + (chips - 1) + (chans - 1))
    low, high = pl.ds(0, cap), pl.ds(cap, cap)
    rows = [
        remote(outgoing.at[low], outer.at[high], row_send.at[0], row_recv.at[0], left, chan),
        remote(outgoing.at[high], outer.at[low], row_send.at[1], row_recv.at[1], right, chan),
    ]
    feats = [
        remote(feat_out.at[low], feat_rows.at[high], feat_send.at[0], feat_recv.at[0], left, chan),
        remote(feat_out.at[high], feat_rows.at[low], feat_send.at[1], feat_recv.at[1], right, chan),
    ]
    for copy in rows + feats:
        copy.start()

    turn = eye(width)
    for name in ("nodes", "wrecv", "cot", "source", "receiver"):
        pulls[name].wait()
    tables[:width, :grid] = own
    tables[:width, slots:] = mm_nt(wrecv[...], nodes[...]).astype(BF)
    tables[width:, slots:] = cot[...]

    def one_hot(index, count, step):
        at = index[pl.ds(step * chunk, chunk)].reshape(1, chunk)
        hit = lax.broadcasted_iota(jnp.int32, (count, chunk), 0) == at
        return jnp.where(hit, 1.0, 0.0).astype(BF)

    for step in range(steps):
        hot_recv[step] = one_hot(receiver, mesh_count, step)
        drawn[step] = mm(tables[:, slots:], hot_recv[step])
        hot_src[step] = one_hot(source, slots, step)
        drawn[step, :width, :] += mm(tables[:width, :grid], hot_src[step, :grid, :])
    for copy in rows:
        copy.wait_recv()
    tables[:width, grid:slots] = mm_nt(turn, outer[...]).astype(BF)

    for step in range(steps):
        pre = drawn[step, :width, :] + mm(tables[:width, grid:slots], hot_src[step, grid:, :])
        gate = sigmoid(pre)
        message = pre * gate
        grad = (drawn[step, width:, :] * (gate + message * (1.0 - gate))).astype(BF)
        pairs[step, :width, :] = message.astype(BF)
        pairs[step, width:, :] = grad
        mine = mm_nt(grad, hot_src[step])
        if step == 0:
            acc[...] = mine
        else:
            acc[...] += mine
    total[...] = acc[...].astype(BF)

    for copy in feats:
        copy.wait_recv()
    pre = mm(feat_rows[:, :inputs], embed[...])
    gate = sigmoid(pre)
    silu = pre * gate
    latent_rows[...] = silu.astype(BF)
    slope_rows[...] = gate + silu * (1.0 - gate)
    back = (mm_tn(wsend[...], total[:, :grid]) * slope[...]).astype(BF)
    back_rows = (mm_tn(total[:, grid:], wsend[...]) * slope_rows[...]).astype(BF)

    def partial(lo, hi):
        return mm_nt(back, feat[lo:hi, :]) + mm_tn(back_rows, feat_rows[:, lo:hi])

    def receiver_sums():
        sums = mm_nt(pairs[0], hot_recv[0])
        for step in range(1, steps):
            sums += mm_nt(pairs[step], hot_recv[step])
        mesh_out[...] = sums[:width].astype(BF)
        e_own[:, :latents] = mm(sums[width:].astype(BF), nodes[...])
        e_own[:, latents:] = mm_nt(total[:, :grid], latent[...]) + mm(total[:, grid:], latent_rows[...])

    part_copies = [
        remote(part_out.at[at], part_in.at[at], part_send.at[at], part_recv.at[at], mate, chan)
        for at in range(len(cuts))
    ]
    e_copy = remote(e_out, e_in, e_send.at[0], e_recv.at[0], mate, chan)
    final_copies = [
        remote(final.at[at], final.at[at], final_send.at[at], final_recv.at[at], mate, chan)
        for at in range(len(cuts))
    ]
    ef_copy = remote(e_final, e_final, ef_send.at[0], ef_recv.at[0], mate, chan)

    @pl.when(core == 0)
    def _():
        for at, (lo, hi) in enumerate(cuts):
            if hi - lo < LANES:
                part_out[at] = jnp.zeros_like(part_out[at])
            part_out[at, :, : hi - lo] = partial(lo, hi).astype(BF)
            part_copies[at].start()
        receiver_sums()
        e_copy.wait_recv()
        e_planes[chip] = (e_own[...] + e_in[...].astype(F32)).astype(BF)
        copies = [
            remote(e_planes.at[chip], e_planes.at[chip], ep_send.at[at], ep_recv.at[at], peer, chan)
            for at, peer in enumerate(peers)
        ]
        for copy in copies:
            copy.start()
        for copy in copies:
            copy.wait_recv()
        value = e_planes[0].astype(F32)
        for at in range(1, chips):
            value += e_planes[at].astype(F32)
        e_final[...] = value
        ef_copy.start()
        for at, (lo, hi) in enumerate(cuts):
            final_copies[at].wait_recv()
            late_out[:, lo:hi] = final[at, :, : hi - lo]
        for copy in part_copies + copies + [ef_copy]:
            copy.wait_send()

    @pl.when(core == 1)
    def _():
        mine = pl.ds(pl.multiple_of(chan * width, width), width)
        for at, (lo, hi) in enumerate(cuts):
            part_own[at, :, : hi - lo] = partial(lo, hi)
        receiver_sums()
        e_out[...] = e_own[...].astype(BF)
        e_copy.start()
        moves = []
        for at, (lo, hi) in enumerate(cuts):
            part_copies[at].wait_recv()
            if hi - lo < LANES:
                z_out[at] = jnp.zeros_like(z_out[at])
            wide = slice(0, hi - lo)
            z_out[at, :, wide] = (part_own[at, :, wide] + part_in[at, :, wide].astype(F32)).astype(BF)
            moves.append([])
            for step, peer in enumerate(others):
                block = pl.ds(pl.multiple_of(peer * width, width), width)
                copy = remote(
                    z_out.at[at, block], z_in.at[at, step], z_send.at[at, step], z_recv.at[at, step], band, peer
                )
                copy.start()
                moves[at].append(copy)
        swaps = []
        for at, (lo, hi) in enumerate(cuts):
            value = z_out[at, mine, :].astype(F32)
            for step, copy in enumerate(moves[at]):
                copy.wait_recv()
                value += z_in[at, step].astype(F32)
            planes[at, chip] = value.astype(BF)
            swaps.append([])
            for step, peer in enumerate(peers):
                copy = remote(
                    planes.at[at, chip], planes.at[at, chip], plane_send.at[at, step], plane_recv.at[at, step],
                    peer, chan,
                )
                copy.start()
                swaps[at].append(copy)
        for at, (lo, hi) in enumerate(cuts):
            for copy in swaps[at]:
                copy.wait_recv()
            value = planes[at, 0].astype(F32)
            for other in range(1, chips):
                value += planes[at, other].astype(F32)
            final[at] = value
            final_copies[at].start()
            late_out[:, lo:hi] = value[:, : hi - lo]
        ef_copy.wait_recv()
        for copy in [e_copy] + final_copies + sum(moves, []) + sum(swaps, []):
            copy.wait_send()

    recv_out[...] = e_final[:, :latents]
    send_out[...] = e_final[:, latents:]
    for copy in rows + feats:
        copy.wait_send()


def place(count, *refs):
    sems = refs[2 * count]
    copies = [
        pltpu.make_async_copy(refs[at], refs[count + at], sems.at[at]) for at in range(count)
    ]
    for copy in copies:
        copy.start()
    for copy in copies:
        copy.wait()


def on_device(
    grid_feat, w_embed, w_send, w_recv, mesh_nodes, mesh_cot, send_index, edge_source, edge_receiver
):
    bands = lax.axis_size("band")
    chans = lax.axis_size("chan")
    chips = bands // 2
    grid, inputs = grid_feat.shape
    latents, width = w_send.shape
    mesh_count = mesh_nodes.shape[0]
    cap = send_index.shape[2]
    slots = grid + 2 * cap
    edges = edge_source.shape[0]
    chunk = math.gcd(edges, 1024)
    steps = edges // chunk
    cuts = -(-inputs // LANES)
    wide = cuts * LANES
    vmem = pl.BlockSpec(memory_space=pltpu.VMEM)
    arrays = (
        grid_feat.T, w_embed, w_send.T, w_recv.T, mesh_nodes, mesh_cot.T,
        send_index, edge_source, edge_receiver,
    )
    scratch = [
        ((latents, grid), BF),
        ((latents, grid), F32),
        ((2 * cap, width), BF),
        ((2 * cap, width), BF),
        ((2 * cap, wide), BF),
        ((2 * cap, wide), BF),
        ((2 * cap, latents), BF),
        ((2 * cap, latents), F32),
        ((2 * width, slots + mesh_count), BF),
        ((steps, mesh_count, chunk), BF),
        ((steps, slots, chunk), BF),
        ((steps, 2 * width, chunk), F32),
        ((steps, 2 * width, chunk), BF),
        ((width, slots), F32),
        ((width, slots), BF),
        ((cuts, latents, LANES), F32),
        ((cuts, latents, LANES), BF),
        ((cuts, latents, LANES), BF),
        ((cuts, latents, LANES), BF),
        ((cuts, chans - 1, width, LANES), BF),
        ((cuts, chips, width, LANES), BF),
        ((cuts, width, LANES), F32),
        ((width, 2 * latents), F32),
        ((width, 2 * latents), BF),
        ((width, 2 * latents), BF),
        ((chips, width, 2 * latents), BF),
        ((width, 2 * latents), F32),
    ]
    sems = [
        (2,), (2,), (2,), (2,), (cuts,), (cuts,), (cuts, chans - 1), (cuts, chans - 1),
        (cuts, chips - 1), (cuts, chips - 1), (cuts,), (cuts,), (1,), (1,), (chips - 1,), (chips - 1,), (1,), (1,),
    ]
    outs = pl.pallas_call(
        functools.partial(body, bands, chans, chunk),
        out_shape=(
            pltpu.VMEM((width, mesh_count), BF),
            pltpu.VMEM((width, inputs), F32),
            pltpu.VMEM((width, latents), F32),
            pltpu.VMEM((width, latents), F32),
        ),
        in_specs=[pl.BlockSpec(memory_space=pl.ANY)] * 9,
        out_specs=(vmem,) * 4,
        scratch_shapes=[pltpu.VMEM(array.shape, array.dtype) for array in arrays]
        + [pltpu.SemaphoreType.DMA((9,))]
        + [pltpu.VMEM(shape, kind) for shape, kind in scratch]
        + [pltpu.SemaphoreType.DMA(shape) for shape in sems],
        compiler_params=pltpu.CompilerParams(collective_id=0, has_side_effects=True),
    )(*arrays)
    anywhere = pl.BlockSpec(memory_space=pl.ANY)
    placed = pl.pallas_call(
        functools.partial(place, len(outs)),
        out_shape=tuple(jax.ShapeDtypeStruct(out.shape, out.dtype) for out in outs),
        in_specs=[vmem] * len(outs),
        out_specs=(anywhere,) * len(outs),
        scratch_shapes=[pltpu.SemaphoreType.DMA((len(outs),))],
    )(*(pltpu.with_memory_space_constraint(out, pltpu.VMEM) for out in outs))
    return tuple(out.T for out in placed)


def solution(mesh):
    placed = (
        P("band", None),
        P(),
        P(None, "chan"),
        P(None, "chan"),
        P("band", None),
        P("band", "chan"),
        P("band", None, None),
        P("band"),
        P("band"),
    )
    return jax.shard_map(
        on_device,
        mesh=mesh,
        in_specs=placed,
        out_specs=(P("band", "chan"), P(None, "chan"), P(None, "chan"), P(None, "chan")),
        check_vma=False,
    )
```

```python
import functools
import math

import jax
import jax.numpy as jnp
from jax import lax
from jax.experimental import pallas as pl
from jax.experimental.pallas import tpu as pltpu
from jax.sharding import PartitionSpec as P

BF = jnp.bfloat16
F32 = jnp.float32
MESH = pl.DeviceIdType.MESH
LANES = 128


def mm(a, b):
    return lax.dot_general(a, b, (((1,), (0,)), ((), ())), preferred_element_type=F32)


def mm_tn(a, b):
    return lax.dot_general(a, b, (((0,), (0,)), ((), ())), preferred_element_type=F32)


def mm_nt(a, b):
    return lax.dot_general(a, b, (((1,), (1,)), ((), ())), preferred_element_type=F32)


def eye(size):
    row = lax.broadcasted_iota(jnp.int32, (size, size), 0)
    col = lax.broadcasted_iota(jnp.int32, (size, size), 1)
    return jnp.where(row == col, 1.0, 0.0).astype(BF)


def sigmoid(v):
    return 0.5 + 0.5 * jnp.tanh(0.5 * v)


def body(
    bands, chans, chunk,
    feat_in, embed_in, wsend_in, wrecv_in, nodes_in, cot_in, send_in, source_in, receiver_in,
    mesh_out, late_out, send_out, recv_out,
    feat, embed, wsend, wrecv, nodes, cot, send, source, receiver, loads,
    embed_t, wsend_t, latent, slope, back, outgoing, outer, feat_out, feat_rows,
    tables, hot_recv, hot_src, drawn, pairs, acc, total,
    part_own, part_out, part_in, z_out, z_in, planes, final,
    e_out, e_in, e_planes, e_final,
    row_send, row_recv, feat_send, feat_recv, part_send, part_recv, z_send, z_recv,
    plane_send, plane_recv, final_send, final_recv, e_send, e_recv, ep_send, ep_recv, ef_send, ef_recv,
):
    band = lax.axis_index("band")
    chan = lax.axis_index("chan")
    chips = bands // 2
    core = lax.rem(band, 2)
    chip = lax.div(band, 2)
    width = wsend.shape[0]
    grid = feat.shape[1]
    inputs = feat.shape[0]
    latents = embed.shape[1]
    mesh_count = nodes.shape[0]
    cap = outgoing.shape[0] // 2
    slots = grid + 2 * cap
    steps = source.shape[0] // chunk
    cuts = [(at, min(at + LANES, inputs)) for at in range(0, inputs, LANES)]
    left = lax.rem(band + bands - 1, bands)
    right = lax.rem(band + 1, bands)
    mate = band + 1 - 2 * core
    peers = [2 * lax.rem(chip + step, chips) + core for step in range(1, chips)]
    others = [lax.rem(chan + step, chans) for step in range(1, chans)]
    ordered = [step + lax.min(lax.max(step + 1 - chan, 0), 1) for step in range(chans - 1)]

    pulls = {}
    for at, (name, src, dst) in enumerate(
        (
            ("send", send_in, send), ("feat", feat_in, feat), ("embed", embed_in, embed),
            ("wsend", wsend_in, wsend), ("nodes", nodes_in, nodes), ("wrecv", wrecv_in, wrecv),
            ("cot", cot_in, cot), ("source", source_in, source), ("receiver", receiver_in, receiver),
        )
    ):
        pulls[name] = pltpu.make_async_copy(src, dst, loads.at[at])
        pulls[name].start()

    barrier = pltpu.get_barrier_semaphore()
    for peer in [left, right, mate] + peers:
        pl.semaphore_signal(barrier, inc=1, device_id=(peer, chan), device_id_type=MESH)
    for peer in others:
        pl.semaphore_signal(barrier, inc=1, device_id=(band, peer), device_id_type=MESH)

    def remote(src, dst, send_sem, recv_sem, to_band, to_chan):
        return pltpu.make_async_remote_copy(
            src_ref=src, dst_ref=dst, send_sem=send_sem, recv_sem=recv_sem,
            device_id=(to_band, to_chan), device_id_type=MESH,
        )

    pulls["send"].wait()
    picks = lax.broadcasted_iota(jnp.int32, (grid, 2 * cap), 0) == jnp.concatenate(
        [send[0, 0:1, :], send[0, 1:2, :]], axis=1
    )
    pick_rows = jnp.transpose(jnp.where(picks, 1.0, 0.0)).astype(BF)
    pulls["feat"].wait()
    pulls["embed"].wait()
    pre = mm_tn(embed[...], feat[...])
    gate = sigmoid(pre)
    silu = pre * gate
    latent[:, :grid] = silu.astype(BF)
    pulls["wsend"].wait()
    own = mm(wsend[...], latent[:, :grid]).astype(BF)
    outgoing[...] = mm_nt(pick_rows, own).astype(BF)
    pl.semaphore_wait(barrier, 3 + (chips - 1) + (chans - 1))
    low, high = pl.ds(0, cap), pl.ds(cap, cap)
    rows = [
        remote(outgoing.at[low], outer.at[high], row_send.at[0], row_recv.at[0], left, chan),
        remote(outgoing.at[high], outer.at[low], row_send.at[1], row_recv.at[1], right, chan),
    ]
    for copy in rows:
        copy.start()
    if inputs < feat_out.shape[1]:
        feat_out[...] = jnp.zeros_like(feat_out)
    feat_out[:, :inputs] = mm_nt(pick_rows, feat[...]).astype(BF)
    feats = [
        remote(feat_out.at[low], feat_rows.at[high], feat_send.at[0], feat_recv.at[0], left, chan),
        remote(feat_out.at[high], feat_rows.at[low], feat_send.at[1], feat_recv.at[1], right, chan),
    ]
    for copy in feats:
        copy.start()

    slope[:, :grid] = gate + silu * (1.0 - gate)
    wsend_t[...] = mm_nt(eye(latents), wsend[...]).astype(BF)
    turn = eye(width)
    for name in ("nodes", "wrecv", "cot", "source", "receiver"):
        pulls[name].wait()
    tables[:width, :grid] = own
    tables[:width, slots:] = mm_nt(wrecv[...], nodes[...]).astype(BF)
    tables[width:, slots:] = cot[...]

    def one_hot(index, count, step):
        at = index[pl.ds(step * chunk, chunk)].reshape(1, chunk)
        hit = lax.broadcasted_iota(jnp.int32, (count, chunk), 0) == at
        return jnp.where(hit, 1.0, 0.0).astype(jnp.float8_e4m3fn)

    for step in range(steps):
        hot_recv[step] = one_hot(receiver, mesh_count, step)
        drawn[step] = mm(tables[:, slots:], hot_recv[step])
        hot_src[step] = one_hot(source, slots, step)
        drawn[step, :width, :] += mm(tables[:width, :grid], hot_src[step, :grid, :])
    embed_t[...] = jnp.transpose(embed[...])
    for copy in rows:
        copy.wait_recv()
    tables[:width, grid:slots] = mm_nt(turn, outer[...]).astype(BF)

    for step in range(steps):
        pre = drawn[step, :width, :] + mm(tables[:width, grid:slots], hot_src[step, grid:, :])
        gate = sigmoid(pre)
        message = pre * gate
        grad = (drawn[step, width:, :] * (gate + message * (1.0 - gate))).astype(BF)
        pairs[step, :width, :] = message.astype(BF)
        pairs[step, width:, :] = grad
        mine = mm_nt(grad, hot_src[step])
        if step == 0:
            acc[...] = mine
        else:
            acc[...] += mine
    total[...] = acc[...].astype(BF)

    for copy in feats:
        copy.wait_recv()
    pre = mm_nt(embed_t[...], feat_rows[:, :inputs])
    gate = sigmoid(pre)
    silu = pre * gate
    latent[:, grid:] = silu.astype(BF)
    slope[:, grid:] = gate + silu * (1.0 - gate)

    def gradients():
        back[...] = (mm(wsend_t[...], total[...]) * slope[...]).astype(BF)

    def partial(lo, hi):
        return mm_nt(back[:, :grid], feat[lo:hi, :]) + mm(back[:, grid:], feat_rows[:, lo:hi])

    def sender_part():
        return mm_nt(total[...], latent[...])

    def receiver_part():
        sums = mm_nt(pairs[0], hot_recv[0])
        for step in range(1, steps):
            sums += mm_nt(pairs[step], hot_recv[step])
        mesh_out[...] = sums[:width].astype(BF)
        return mm(sums[width:].astype(BF), nodes[...])

    part_copies = [
        remote(part_out.at[at], part_in.at[at], part_send.at[at], part_recv.at[at], mate, chan)
        for at in range(len(cuts))
    ]
    sides = ((sender_part, send_out), (receiver_part, recv_out))
    e_copies = [
        remote(e_out.at[at], e_in.at[at], e_send.at[at], e_recv.at[at], mate, chan) for at in range(2)
    ]
    ef_copies = [
        remote(e_final.at[at], e_final.at[at], ef_send.at[at], ef_recv.at[at], mate, chan) for at in range(2)
    ]
    final_copies = [
        remote(final.at[at], final.at[at], final_send.at[at], final_recv.at[at], mate, chan)
        for at in range(len(cuts))
    ]

    @pl.when(core == 0)
    def _():
        gradients()
        for at, (lo, hi) in enumerate(cuts):
            if hi - lo < LANES:
                part_out[at] = jnp.zeros_like(part_out[at])
            part_out[at, :, : hi - lo] = partial(lo, hi).astype(BF)
            part_copies[at].start()
        copies = []
        for side, (own_part, _) in enumerate(sides):
            value = own_part()
            e_copies[side].wait_recv()
            e_planes[side, chip] = (value + e_in[side].astype(F32)).astype(BF)
            copies.append([])
            for at, peer in enumerate(peers):
                copy = remote(
                    e_planes.at[side, chip], e_planes.at[side, chip], ep_send.at[side, at], ep_recv.at[side, at],
                    peer, chan,
                )
                copy.start()
                copies[side].append(copy)
        for side, (_, out) in enumerate(sides):
            for copy in copies[side]:
                copy.wait_recv()
            value = e_planes[side, 0].astype(F32)
            for at in range(1, chips):
                value += e_planes[side, at].astype(F32)
            e_final[side] = value
            ef_copies[side].start()
            out[...] = value
        for at, (lo, hi) in enumerate(cuts):
            final_copies[at].wait_recv()
            late_out[:, lo:hi] = final[at, :, : hi - lo]
        for copy in part_copies + sum(copies, []) + ef_copies:
            copy.wait_send()

    @pl.when(core == 1)
    def _():
        mine = pl.ds(pl.multiple_of(chan * width, width), width)
        first = pl.ds(pl.multiple_of(ordered[0] * width, width), width)
        e_out[0] = sender_part().astype(BF)
        e_copies[0].start()
        gradients()
        for at, (lo, hi) in enumerate(cuts):
            part_own[at, :, : hi - lo] = partial(lo, hi)
        e_out[1] = receiver_part().astype(BF)
        e_copies[1].start()
        moves = []
        for at, (lo, hi) in enumerate(cuts):
            part_copies[at].wait_recv()
            if hi - lo < LANES:
                z_out[at] = jnp.zeros_like(z_out[at])
            wide = slice(0, hi - lo)
            z_out[at, :, wide] = (part_own[at, :, wide] + part_in[at, :, wide].astype(F32)).astype(BF)
            copy = remote(
                z_out.at[at, first], z_in.at[at, chan], z_send.at[at, 0], z_recv.at[at, chan], band, ordered[0]
            )
            copy.start()
            moves.append(copy)
        for step, peer in enumerate(ordered[1:], 1):
            block = pl.ds(pl.multiple_of(peer * width, width), width)
            for at in range(len(cuts)):
                copy = remote(
                    z_out.at[at, block], z_in.at[at, chan], z_send.at[at, step], z_recv.at[at, chan], band, peer
                )
                copy.start()
                moves.append(copy)
        swaps = []
        for at, (lo, hi) in enumerate(cuts):
            value = z_out[at, mine, :].astype(F32)
            for step, peer in enumerate(ordered):
                remote(
                    z_out.at[at, mine], z_in.at[at, peer], z_send.at[at, step], z_recv.at[at, peer], band, peer
                ).wait_recv()
                value += z_in[at, peer].astype(F32)
            planes[at, chip] = value.astype(BF)
            swaps.append([])
            for step, peer in enumerate(peers):
                copy = remote(
                    planes.at[at, chip], planes.at[at, chip], plane_send.at[at, step], plane_recv.at[at, step],
                    peer, chan,
                )
                copy.start()
                swaps[at].append(copy)
        for at, (lo, hi) in enumerate(cuts):
            for copy in swaps[at]:
                copy.wait_recv()
            value = planes[at, 0].astype(F32)
            for other in range(1, chips):
                value += planes[at, other].astype(F32)
            final[at] = value
            final_copies[at].start()
            late_out[:, lo:hi] = value[:, : hi - lo]
        for side, (_, out) in enumerate(sides):
            ef_copies[side].wait_recv()
            out[...] = e_final[side]
        for copy in e_copies + final_copies + moves + sum(swaps, []):
            copy.wait_send()

    for copy in rows + feats:
        copy.wait_send()


def place(count, *refs):
    sems = refs[2 * count]
    copies = [
        pltpu.make_async_copy(refs[at], refs[count + at], sems.at[at]) for at in range(count)
    ]
    for copy in copies:
        copy.start()
    for copy in copies:
        copy.wait()


def on_device(
    grid_feat, w_embed, w_send, w_recv, mesh_nodes, mesh_cot, send_index, edge_source, edge_receiver
):
    bands = lax.axis_size("band")
    chans = lax.axis_size("chan")
    chips = bands // 2
    grid, inputs = grid_feat.shape
    latents, width = w_send.shape
    mesh_count = mesh_nodes.shape[0]
    cap = send_index.shape[2]
    slots = grid + 2 * cap
    edges = edge_source.shape[0]
    chunk = math.gcd(edges, 1024)
    steps = edges // chunk
    cuts = -(-inputs // LANES)
    wide = cuts * LANES
    vmem = pl.BlockSpec(memory_space=pltpu.VMEM)
    arrays = (
        grid_feat.T, w_embed, w_send.T, w_recv.T, mesh_nodes, mesh_cot.T,
        send_index, edge_source, edge_receiver,
    )
    scratch = [
        ((latents, inputs), BF),
        ((latents, width), BF),
        ((latents, slots), BF),
        ((latents, slots), F32),
        ((latents, slots), BF),
        ((2 * cap, width), BF),
        ((2 * cap, width), BF),
        ((2 * cap, wide), BF),
        ((2 * cap, wide), BF),
        ((2 * width, slots + mesh_count), BF),
        ((steps, mesh_count, chunk), jnp.float8_e4m3fn),
        ((steps, slots, chunk), jnp.float8_e4m3fn),
        ((steps, 2 * width, chunk), F32),
        ((steps, 2 * width, chunk), BF),
        ((width, slots), F32),
        ((width, slots), BF),
        ((cuts, latents, LANES), F32),
        ((cuts, latents, LANES), BF),
        ((cuts, latents, LANES), BF),
        ((cuts, latents, LANES), BF),
        ((cuts, chans, width, LANES), BF),
        ((cuts, chips, width, LANES), BF),
        ((cuts, width, LANES), F32),
        ((2, width, latents), BF),
        ((2, width, latents), BF),
        ((2, chips, width, latents), BF),
        ((2, width, latents), F32),
    ]
    sems = [
        (2,), (2,), (2,), (2,), (cuts,), (cuts,), (cuts, chans - 1), (cuts, chans),
        (cuts, chips - 1), (cuts, chips - 1), (cuts,), (cuts,), (2,), (2,), (2, chips - 1), (2, chips - 1), (2,), (2,),
    ]
    outs = pl.pallas_call(
        functools.partial(body, bands, chans, chunk),
        out_shape=(
            pltpu.VMEM((width, mesh_count), BF),
            pltpu.VMEM((width, inputs), F32),
            pltpu.VMEM((width, latents), F32),
            pltpu.VMEM((width, latents), F32),
        ),
        in_specs=[pl.BlockSpec(memory_space=pl.ANY)] * 9,
        out_specs=(vmem,) * 4,
        scratch_shapes=[pltpu.VMEM(array.shape, array.dtype) for array in arrays]
        + [pltpu.SemaphoreType.DMA((9,))]
        + [pltpu.VMEM(shape, kind) for shape, kind in scratch]
        + [pltpu.SemaphoreType.DMA(shape) for shape in sems],
        compiler_params=pltpu.CompilerParams(collective_id=0, has_side_effects=True),
    )(*arrays)
    anywhere = pl.BlockSpec(memory_space=pl.ANY)
    placed = pl.pallas_call(
        functools.partial(place, len(outs)),
        out_shape=tuple(jax.ShapeDtypeStruct(out.shape, out.dtype) for out in outs),
        in_specs=[vmem] * len(outs),
        out_specs=(anywhere,) * len(outs),
        scratch_shapes=[pltpu.SemaphoreType.DMA((len(outs),))],
    )(*(pltpu.with_memory_space_constraint(out, pltpu.VMEM) for out in outs))
    return tuple(out.T for out in placed)


def solution(mesh):
    placed = (
        P("band", None),
        P(),
        P(None, "chan"),
        P(None, "chan"),
        P("band", None),
        P("band", "chan"),
        P("band", None, None),
        P("band"),
        P("band"),
    )
    return jax.shard_map(
        on_device,
        mesh=mesh,
        in_specs=placed,
        out_specs=(P("band", "chan"), P(None, "chan"), P(None, "chan"), P(None, "chan")),
        check_vma=False,
    )
```

```python
import functools
import math

import jax
import jax.numpy as jnp
from jax import lax
from jax.experimental import pallas as pl
from jax.experimental.pallas import tpu as pltpu
from jax.sharding import PartitionSpec as P

BF = jnp.bfloat16
F32 = jnp.float32
MESH = pl.DeviceIdType.MESH
LANES = 128


def mm(a, b):
    return lax.dot_general(a, b, (((1,), (0,)), ((), ())), preferred_element_type=F32)


def mm_tn(a, b):
    return lax.dot_general(a, b, (((0,), (0,)), ((), ())), preferred_element_type=F32)


def mm_nt(a, b):
    return lax.dot_general(a, b, (((1,), (1,)), ((), ())), preferred_element_type=F32)


def eye(size):
    row = lax.broadcasted_iota(jnp.int32, (size, size), 0)
    col = lax.broadcasted_iota(jnp.int32, (size, size), 1)
    return jnp.where(row == col, 1.0, 0.0).astype(BF)


def sigmoid(v):
    return 0.5 + 0.5 * jnp.tanh(0.5 * v)


def body(
    bands, chans, chunk,
    feat_in, embed_in, wsend_in, wrecv_in, nodes_in, cot_in, send_in, source_in, receiver_in,
    mesh_out, late_out, send_out, recv_out,
    feat, embed, wsend, wrecv, nodes, cot, send, source, receiver, loads,
    embed_t, wsend_t, latent, slope, back, outgoing, outer, feat_out, feat_rows,
    tables, hot_recv, hot_src, drawn, pairs, acc, total,
    part_own, part_out, part_in, z_out, z_in, planes, final,
    e_out, e_in, e_planes, e_final,
    row_send, row_recv, feat_send, feat_recv, part_send, part_recv, z_send, z_recv,
    plane_send, plane_recv, final_send, final_recv, e_send, e_recv, ep_send, ep_recv, ef_send, ef_recv,
):
    band = lax.axis_index("band")
    chan = lax.axis_index("chan")
    chips = bands // 2
    core = lax.rem(band, 2)
    chip = lax.div(band, 2)
    width = wsend.shape[0]
    grid = feat.shape[1]
    inputs = feat.shape[0]
    latents = embed.shape[1]
    mesh_count = nodes.shape[0]
    cap = outgoing.shape[0] // 2
    slots = grid + 2 * cap
    steps = source.shape[0] // chunk
    cuts = [(at, min(at + LANES, inputs)) for at in range(0, inputs, LANES)]
    left = lax.rem(band + bands - 1, bands)
    right = lax.rem(band + 1, bands)
    mate = band + 1 - 2 * core
    peers = [2 * (step + lax.min(lax.max(step + 1 - chip, 0), 1)) + core for step in range(chips - 1)]
    others = [lax.rem(chan + step, chans) for step in range(1, chans)]
    ordered = [step + lax.min(lax.max(step + 1 - chan, 0), 1) for step in range(chans - 1)]

    pulls = {}
    for at, (name, src, dst) in enumerate(
        (
            ("send", send_in, send), ("feat", feat_in, feat), ("embed", embed_in, embed),
            ("wsend", wsend_in, wsend), ("nodes", nodes_in, nodes), ("wrecv", wrecv_in, wrecv),
            ("cot", cot_in, cot), ("source", source_in, source), ("receiver", receiver_in, receiver),
        )
    ):
        pulls[name] = pltpu.make_async_copy(src, dst, loads.at[at])
        pulls[name].start()

    barrier = pltpu.get_barrier_semaphore()
    for peer in [left, right, mate] + peers:
        pl.semaphore_signal(barrier, inc=1, device_id=(peer, chan), device_id_type=MESH)
    for peer in others:
        pl.semaphore_signal(barrier, inc=1, device_id=(band, peer), device_id_type=MESH)

    def remote(src, dst, send_sem, recv_sem, to_band, to_chan):
        return pltpu.make_async_remote_copy(
            src_ref=src, dst_ref=dst, send_sem=send_sem, recv_sem=recv_sem,
            device_id=(to_band, to_chan), device_id_type=MESH,
        )

    pulls["send"].wait()
    picks = lax.broadcasted_iota(jnp.int32, (grid, 2 * cap), 0) == jnp.concatenate(
        [send[0, 0:1, :], send[0, 1:2, :]], axis=1
    )
    pick_rows = jnp.transpose(jnp.where(picks, 1.0, 0.0)).astype(BF)
    low, high = pl.ds(0, cap), pl.ds(cap, cap)

    @pl.when(band == 0)
    def _():
        outer[low, :] = jnp.zeros((cap, width), BF)
        feat_rows[low, :] = jnp.zeros((cap, feat_rows.shape[1]), BF)

    @pl.when(band == bands - 1)
    def _():
        outer[high, :] = jnp.zeros((cap, width), BF)
        feat_rows[high, :] = jnp.zeros((cap, feat_rows.shape[1]), BF)

    pulls["feat"].wait()
    if inputs < feat_out.shape[1]:
        feat_out[...] = jnp.zeros_like(feat_out)
    listed = mm_nt(pick_rows, feat[...]).astype(BF)
    feat_out[:, :inputs] = listed
    pulls["embed"].wait()
    pre = mm(listed, embed[...])
    listed = (pre * sigmoid(pre)).astype(BF)
    pulls["wsend"].wait()
    outgoing[...] = mm_nt(listed, wsend[...]).astype(BF)
    pl.semaphore_wait(barrier, 3 + (chips - 1) + (chans - 1))
    rows = [
        remote(outgoing.at[low], outer.at[high], row_send.at[0], row_recv.at[0], left, chan),
        remote(outgoing.at[high], outer.at[low], row_send.at[1], row_recv.at[1], right, chan),
    ]
    feats = [
        remote(feat_out.at[low], feat_rows.at[high], feat_send.at[0], feat_recv.at[0], left, chan),
        remote(feat_out.at[high], feat_rows.at[low], feat_send.at[1], feat_recv.at[1], right, chan),
    ]
    has_left, has_right = band > 0, band < bands - 1

    @pl.when(has_left)
    def _():
        rows[0].start()
        feats[0].start()

    @pl.when(has_right)
    def _():
        rows[1].start()
        feats[1].start()


    embed_t[...] = jnp.transpose(embed[...])
    pre = mm(embed_t[...], feat[...])
    gate = sigmoid(pre)
    silu = pre * gate
    latent[:, :grid] = silu.astype(BF)
    own = mm(wsend[...], latent[:, :grid]).astype(BF)
    slope[:, :grid] = gate + silu * (1.0 - gate)
    wsend_t[...] = mm_nt(eye(latents), wsend[...]).astype(BF)
    turn = eye(width)
    for name in ("nodes", "wrecv", "cot", "source", "receiver"):
        pulls[name].wait()
    tables[:width, :grid] = own
    tables[:width, slots:] = mm_nt(wrecv[...], nodes[...]).astype(BF)
    tables[width:, slots:] = cot[...]

    def one_hot(index, count, step):
        at = index[pl.ds(step * chunk, chunk)].reshape(1, chunk)
        hit = lax.broadcasted_iota(jnp.int32, (count, chunk), 0) == at
        return jnp.where(hit, 1.0, 0.0).astype(jnp.float8_e4m3fn)

    for step in range(steps):
        hot_recv[step] = one_hot(receiver, mesh_count, step)
        drawn[step] = mm(tables[:, slots:], hot_recv[step])
        hot_src[step] = one_hot(source, slots, step)
        drawn[step, :width, :] += mm(tables[:width, :grid], hot_src[step, :grid, :])
    pl.when(has_right)(rows[0].wait_recv)
    pl.when(has_left)(rows[1].wait_recv)
    tables[:width, grid:slots] = mm_nt(turn, outer[...]).astype(BF)

    for step in range(steps):
        pre = drawn[step, :width, :] + mm(tables[:width, grid:slots], hot_src[step, grid:, :])
        gate = sigmoid(pre)
        message = pre * gate
        grad = (drawn[step, width:, :] * (gate + message * (1.0 - gate))).astype(BF)
        pairs[step, :width, :] = message.astype(BF)
        pairs[step, width:, :] = grad
        mine = mm_nt(grad, hot_src[step])
        if step == 0:
            acc[...] = mine
        else:
            acc[...] += mine
    total[...] = acc[...].astype(BF)

    def finish_rows():
        pl.when(has_right)(feats[0].wait_recv)
        pl.when(has_left)(feats[1].wait_recv)
        pre = mm_nt(embed_t[...], feat_rows[:, :inputs])
        gate = sigmoid(pre)
        silu = pre * gate
        latent[:, grid:] = silu.astype(BF)
        slope[:, grid:] = gate + silu * (1.0 - gate)

    def gradients():
        back[...] = (mm(wsend_t[...], total[...]) * slope[...]).astype(BF)

    def partial(lo, hi):
        return mm_nt(back[:, :grid], feat[lo:hi, :]) + mm(back[:, grid:], feat_rows[:, lo:hi])

    def sender_part():
        return mm_nt(total[...], latent[...])

    def receiver_sums(rows):
        sums = mm_nt(pairs[0, rows, :], hot_recv[0])
        for step in range(1, steps):
            sums += mm_nt(pairs[step, rows, :], hot_recv[step])
        return sums.astype(BF)

    def receiver_part():
        return mm(receiver_sums(slice(width, 2 * width)), nodes[...])

    part_copies = [
        remote(part_out.at[at], part_in.at[at], part_send.at[at], part_recv.at[at], mate, chan)
        for at in range(len(cuts))
    ]
    sides = ((sender_part, send_out), (receiver_part, recv_out))
    e_copies = [
        remote(e_out.at[at], e_in.at[at], e_send.at[at], e_recv.at[at], mate, chan) for at in range(2)
    ]
    ef_copies = [
        remote(e_final.at[at], e_final.at[at], ef_send.at[at], ef_recv.at[at], mate, chan) for at in range(2)
    ]
    final_copies = [
        remote(final.at[at], final.at[at], final_send.at[at], final_recv.at[at], mate, chan)
        for at in range(len(cuts))
    ]

    @pl.when(core == 0)
    def _():
        finish_rows()
        gradients()
        for at, (lo, hi) in enumerate(cuts):
            if hi - lo < LANES:
                part_out[at] = jnp.zeros_like(part_out[at])
            part_out[at, :, : hi - lo] = partial(lo, hi).astype(BF)
            part_copies[at].start()
        copies = []
        for side, (own_part, _) in enumerate(sides):
            value = own_part()
            e_copies[side].wait_recv()
            e_planes[side, chip] = (value + e_in[side].astype(F32)).astype(BF)
            copies.append([])
            for at, peer in enumerate(peers):
                copy = remote(
                    e_planes.at[side, chip], e_planes.at[side, chip], ep_send.at[side, at], ep_recv.at[side, chip],
                    peer, chan,
                )
                copy.start()
                copies[side].append(copy)
        mesh_out[...] = receiver_sums(slice(0, width))
        for side, (_, out) in enumerate(sides):
            for at, peer in enumerate(peers):
                slot = lax.div(peer, 2)
                remote(
                    e_planes.at[side, slot], e_planes.at[side, slot], ep_send.at[side, at], ep_recv.at[side, slot],
                    peer, chan,
                ).wait_recv()
            value = e_planes[side, 0].astype(F32)
            for at in range(1, chips):
                value += e_planes[side, at].astype(F32)
            e_final[side] = value
            ef_copies[side].start()
            out[...] = value
        for at, (lo, hi) in enumerate(cuts):
            final_copies[at].wait_recv()
            late_out[:, lo:hi] = final[at, :, : hi - lo]
        for copy in part_copies + sum(copies, []) + ef_copies:
            copy.wait_send()

    @pl.when(core == 1)
    def _():
        mine = pl.ds(pl.multiple_of(chan * width, width), width)
        first = pl.ds(pl.multiple_of(ordered[0] * width, width), width)
        finish_rows()
        e_out[0] = sender_part().astype(BF)
        e_copies[0].start()
        gradients()
        for at, (lo, hi) in enumerate(cuts):
            part_own[at, :, : hi - lo] = partial(lo, hi)
        e_out[1] = receiver_part().astype(BF)
        e_copies[1].start()
        moves = []
        for at, (lo, hi) in enumerate(cuts):
            part_copies[at].wait_recv()
            if hi - lo < LANES:
                z_out[at] = jnp.zeros_like(z_out[at])
            wide = slice(0, hi - lo)
            z_out[at, :, wide] = (part_own[at, :, wide] + part_in[at, :, wide].astype(F32)).astype(BF)
            copy = remote(
                z_out.at[at, first], z_in.at[at, chan], z_send.at[at, 0], z_recv.at[at, chan], band, ordered[0]
            )
            copy.start()
            moves.append(copy)
        for step, peer in enumerate(ordered[1:], 1):
            block = pl.ds(pl.multiple_of(peer * width, width), width)
            for at in range(len(cuts)):
                copy = remote(
                    z_out.at[at, block], z_in.at[at, chan], z_send.at[at, step], z_recv.at[at, chan], band, peer
                )
                copy.start()
                moves.append(copy)
        mesh_out[...] = receiver_sums(slice(0, width))
        swaps = []
        for at, (lo, hi) in enumerate(cuts):
            value = z_out[at, mine, :].astype(F32)
            for step, peer in enumerate(ordered):
                remote(
                    z_out.at[at, mine], z_in.at[at, peer], z_send.at[at, step], z_recv.at[at, peer], band, peer
                ).wait_recv()
                value += z_in[at, peer].astype(F32)
            planes[at, chip] = value.astype(BF)
            swaps.append([])
            for step, peer in enumerate(peers):
                copy = remote(
                    planes.at[at, chip], planes.at[at, chip], plane_send.at[at, step], plane_recv.at[at, chip],
                    peer, chan,
                )
                copy.start()
                swaps[at].append(copy)
        for at, (lo, hi) in enumerate(cuts):
            for step, peer in enumerate(peers):
                slot = lax.div(peer, 2)
                remote(
                    planes.at[at, slot], planes.at[at, slot], plane_send.at[at, step], plane_recv.at[at, slot],
                    peer, chan,
                ).wait_recv()
            value = planes[at, 0].astype(F32)
            for other in range(1, chips):
                value += planes[at, other].astype(F32)
            final[at] = value
            final_copies[at].start()
        for side, (_, out) in enumerate(sides):
            ef_copies[side].wait_recv()
            out[...] = e_final[side]
        for at, (lo, hi) in enumerate(cuts):
            late_out[:, lo:hi] = final[at, :, : hi - lo]
        for copy in e_copies + final_copies + moves + sum(swaps, []):
            copy.wait_send()

    for has, at in ((has_left, 0), (has_right, 1)):
        pl.when(has)(rows[at].wait_send)
        pl.when(has)(feats[at].wait_send)


def place(count, *refs):
    sems = refs[2 * count]
    copies = [
        pltpu.make_async_copy(refs[at], refs[count + at], sems.at[at]) for at in range(count)
    ]
    for copy in copies:
        copy.start()
    for copy in copies:
        copy.wait()


def on_device(
    grid_feat, w_embed, w_send, w_recv, mesh_nodes, mesh_cot, send_index, edge_source, edge_receiver
):
    bands = lax.axis_size("band")
    chans = lax.axis_size("chan")
    chips = bands // 2
    grid, inputs = grid_feat.shape
    latents, width = w_send.shape
    mesh_count = mesh_nodes.shape[0]
    cap = send_index.shape[2]
    slots = grid + 2 * cap
    edges = edge_source.shape[0]
    chunk = math.gcd(edges, 2048)
    steps = edges // chunk
    cuts = -(-inputs // LANES)
    wide = cuts * LANES
    vmem = pl.BlockSpec(memory_space=pltpu.VMEM)
    arrays = (
        grid_feat.T, w_embed, w_send.T, w_recv.T, mesh_nodes, mesh_cot.T,
        send_index, edge_source, edge_receiver,
    )
    scratch = [
        ((latents, inputs), BF),
        ((latents, width), BF),
        ((latents, slots), BF),
        ((latents, slots), F32),
        ((latents, slots), BF),
        ((2 * cap, width), BF),
        ((2 * cap, width), BF),
        ((2 * cap, wide), BF),
        ((2 * cap, wide), BF),
        ((2 * width, slots + mesh_count), BF),
        ((steps, mesh_count, chunk), jnp.float8_e4m3fn),
        ((steps, slots, chunk), jnp.float8_e4m3fn),
        ((steps, 2 * width, chunk), F32),
        ((steps, 2 * width, chunk), BF),
        ((width, slots), F32),
        ((width, slots), BF),
        ((cuts, latents, LANES), F32),
        ((cuts, latents, LANES), BF),
        ((cuts, latents, LANES), BF),
        ((cuts, latents, LANES), BF),
        ((cuts, chans, width, LANES), BF),
        ((cuts, chips, width, LANES), BF),
        ((cuts, width, LANES), F32),
        ((2, width, latents), BF),
        ((2, width, latents), BF),
        ((2, chips, width, latents), BF),
        ((2, width, latents), F32),
    ]
    sems = [
        (2,), (2,), (2,), (2,), (cuts,), (cuts,), (cuts, chans - 1), (cuts, chans),
        (cuts, chips - 1), (cuts, chips), (cuts,), (cuts,), (2,), (2,), (2, chips - 1), (2, chips), (2,), (2,),
    ]
    outs = pl.pallas_call(
        functools.partial(body, bands, chans, chunk),
        out_shape=(
            pltpu.VMEM((width, mesh_count), BF),
            pltpu.VMEM((width, inputs), F32),
            pltpu.VMEM((width, latents), F32),
            pltpu.VMEM((width, latents), F32),
        ),
        in_specs=[pl.BlockSpec(memory_space=pl.ANY)] * 9,
        out_specs=(vmem,) * 4,
        scratch_shapes=[pltpu.VMEM(array.shape, array.dtype) for array in arrays]
        + [pltpu.SemaphoreType.DMA((9,))]
        + [pltpu.VMEM(shape, kind) for shape, kind in scratch]
        + [pltpu.SemaphoreType.DMA(shape) for shape in sems],
        compiler_params=pltpu.CompilerParams(collective_id=0, has_side_effects=True),
    )(*arrays)
    anywhere = pl.BlockSpec(memory_space=pl.ANY)
    placed = pl.pallas_call(
        functools.partial(place, len(outs)),
        out_shape=tuple(jax.ShapeDtypeStruct(out.shape, out.dtype) for out in outs),
        in_specs=[vmem] * len(outs),
        out_specs=(anywhere,) * len(outs),
        scratch_shapes=[pltpu.SemaphoreType.DMA((len(outs),))],
    )(*(pltpu.with_memory_space_constraint(out, pltpu.VMEM) for out in outs))
    return tuple(out.T for out in placed)


def solution(mesh):
    placed = (
        P("band", None),
        P(),
        P(None, "chan"),
        P(None, "chan"),
        P("band", None),
        P("band", "chan"),
        P("band", None, None),
        P("band"),
        P("band"),
    )
    return jax.shard_map(
        on_device,
        mesh=mesh,
        in_specs=placed,
        out_specs=(P("band", "chan"), P(None, "chan"), P(None, "chan"), P(None, "chan")),
        check_vma=False,
    )
```

```python
import functools
import math

import jax
import jax.numpy as jnp
from jax import lax
from jax.experimental import pallas as pl
from jax.experimental.pallas import tpu as pltpu
from jax.sharding import PartitionSpec as P

BF = jnp.bfloat16
F32 = jnp.float32
MESH = pl.DeviceIdType.MESH
LANES = 128


def mm(a, b):
    return lax.dot_general(a, b, (((1,), (0,)), ((), ())), preferred_element_type=F32)


def mm_tn(a, b):
    return lax.dot_general(a, b, (((0,), (0,)), ((), ())), preferred_element_type=F32)


def mm_nt(a, b):
    return lax.dot_general(a, b, (((1,), (1,)), ((), ())), preferred_element_type=F32)


def eye(size):
    row = lax.broadcasted_iota(jnp.int32, (size, size), 0)
    col = lax.broadcasted_iota(jnp.int32, (size, size), 1)
    return jnp.where(row == col, 1.0, 0.0).astype(BF)


def sigmoid(v):
    return 0.5 + 0.5 * jnp.tanh(0.5 * v)


def body(
    bands, chans, chunk,
    feat_in, embed_in, wsend_in, wrecv_in, nodes_in, cot_in, send_in, source_in, receiver_in,
    mesh_out, late_out, send_out, recv_out,
    feat, embed, wsend, wrecv, nodes, cot, send, source, receiver, loads,
    embed_t, wsend_t, latent, slope, back, outgoing, outer, feat_out, feat_rows,
    tables, hot_recv, hot_src, drawn, pairs, acc, total,
    part_own, part_out, part_in, z_out, z_in, planes, final,
    e_out, e_in, e_planes, e_final,
    row_send, row_recv, feat_send, feat_recv, part_send, part_recv, z_send, z_recv,
    plane_send, plane_recv, final_send, final_recv, e_send, e_recv, ep_send, ep_recv, ef_send, ef_recv,
):
    band = lax.axis_index("band")
    chan = lax.axis_index("chan")
    chips = bands // 2
    core = lax.rem(band, 2)
    chip = lax.div(band, 2)
    width = wsend.shape[0]
    grid = feat.shape[1]
    inputs = feat.shape[0]
    latents = embed.shape[1]
    mesh_count = nodes.shape[0]
    cap = outgoing.shape[0] // 2
    slots = grid + 2 * cap
    steps = source.shape[0] // chunk
    cuts = [(at, min(at + LANES, inputs)) for at in range(0, inputs, LANES)]
    left = lax.rem(band + bands - 1, bands)
    right = lax.rem(band + 1, bands)
    mate = band + 1 - 2 * core
    peers = [2 * (step + lax.min(lax.max(step + 1 - chip, 0), 1)) + core for step in range(chips - 1)]
    ordered = [step + lax.min(lax.max(step + 1 - chan, 0), 1) for step in range(chans - 1)]

    pulls = {}
    for at, (name, src, dst) in enumerate(
        (
            ("send", send_in, send), ("feat", feat_in, feat), ("embed", embed_in, embed),
            ("wsend", wsend_in, wsend), ("nodes", nodes_in, nodes), ("wrecv", wrecv_in, wrecv),
            ("cot", cot_in, cot), ("source", source_in, source), ("receiver", receiver_in, receiver),
        )
    ):
        pulls[name] = pltpu.make_async_copy(src, dst, loads.at[at])
        pulls[name].start()

    barrier = pltpu.get_barrier_semaphore()
    for peer in [left, right, mate] + peers:
        pl.semaphore_signal(barrier, inc=1, device_id=(peer, chan), device_id_type=MESH)

    @pl.when(core == 1)
    def _():
        for peer in ordered:
            pl.semaphore_signal(barrier, inc=1, device_id=(band, peer), device_id_type=MESH)


    def remote(src, dst, send_sem, recv_sem, to_band, to_chan):
        return pltpu.make_async_remote_copy(
            src_ref=src, dst_ref=dst, send_sem=send_sem, recv_sem=recv_sem,
            device_id=(to_band, to_chan), device_id_type=MESH,
        )

    pulls["send"].wait()
    picks = lax.broadcasted_iota(jnp.int32, (grid, 2 * cap), 0) == jnp.concatenate(
        [send[0, 0:1, :], send[0, 1:2, :]], axis=1
    )
    pick_rows = jnp.transpose(jnp.where(picks, 1.0, 0.0)).astype(BF)
    low, high = pl.ds(0, cap), pl.ds(cap, cap)

    @pl.when(band == 0)
    def _():
        outer[low, :] = jnp.zeros((cap, width), BF)
        feat_rows[low, :] = jnp.zeros((cap, feat_rows.shape[1]), BF)

    @pl.when(band == bands - 1)
    def _():
        outer[high, :] = jnp.zeros((cap, width), BF)
        feat_rows[high, :] = jnp.zeros((cap, feat_rows.shape[1]), BF)

    pulls["feat"].wait()
    if inputs < feat_out.shape[1]:
        feat_out[...] = jnp.zeros_like(feat_out)
    listed = mm_nt(pick_rows, feat[...]).astype(BF)
    feat_out[:, :inputs] = listed
    pulls["embed"].wait()
    pre = mm(listed, embed[...])
    listed = (pre * sigmoid(pre)).astype(BF)
    pulls["wsend"].wait()
    outgoing[...] = mm_nt(listed, wsend[...]).astype(BF)
    pl.semaphore_wait(barrier, 3 + (chips - 1) + core * (chans - 1))
    rows = [
        remote(outgoing.at[low], outer.at[high], row_send.at[0], row_recv.at[0], left, chan),
        remote(outgoing.at[high], outer.at[low], row_send.at[1], row_recv.at[1], right, chan),
    ]
    feats = [
        remote(feat_out.at[low], feat_rows.at[high], feat_send.at[0], feat_recv.at[0], left, chan),
        remote(feat_out.at[high], feat_rows.at[low], feat_send.at[1], feat_recv.at[1], right, chan),
    ]
    has_left, has_right = band > 0, band < bands - 1

    @pl.when(has_left)
    def _():
        rows[0].start()
        feats[0].start()

    @pl.when(has_right)
    def _():
        rows[1].start()
        feats[1].start()


    embed_t[...] = jnp.transpose(embed[...])
    pre = mm(embed_t[...], feat[...])
    gate = sigmoid(pre)
    silu = pre * gate
    latent[:, :grid] = silu.astype(BF)
    own = mm(wsend[...], latent[:, :grid]).astype(BF)
    slope[:, :grid] = gate + silu * (1.0 - gate)
    wsend_t[...] = mm_nt(eye(latents), wsend[...]).astype(BF)
    turn = eye(width)
    for name in ("nodes", "wrecv", "cot", "source", "receiver"):
        pulls[name].wait()
    tables[:width, :grid] = own
    tables[:width, slots:] = mm_nt(wrecv[...], nodes[...]).astype(BF)
    tables[width:, slots:] = cot[...]

    def one_hot(index, count, step):
        at = index[pl.ds(step * chunk, chunk)].reshape(1, chunk)
        hit = lax.broadcasted_iota(jnp.int32, (count, chunk), 0) == at
        return jnp.where(hit, 1.0, 0.0).astype(jnp.float8_e4m3fn)

    for step in range(steps):
        hot_recv[step] = one_hot(receiver, mesh_count, step)
        drawn[step] = mm(tables[:, slots:], hot_recv[step])
        hot_src[step] = one_hot(source, slots, step)
        drawn[step, :width, :] += mm(tables[:width, :grid], hot_src[step, :grid, :])
    pl.when(has_right)(rows[0].wait_recv)
    pl.when(has_left)(rows[1].wait_recv)
    tables[:width, grid:slots] = mm_nt(turn, outer[...]).astype(BF)

    for step in range(steps):
        pre = drawn[step, :width, :] + mm(tables[:width, grid:slots], hot_src[step, grid:, :])
        gate = sigmoid(pre)
        message = pre * gate
        grad = (drawn[step, width:, :] * (gate + message * (1.0 - gate))).astype(BF)
        pairs[step, :width, :] = message.astype(BF)
        pairs[step, width:, :] = grad
        mine = mm_nt(grad, hot_src[step])
        if step == 0:
            acc[...] = mine
        else:
            acc[...] += mine
    total[...] = acc[...].astype(BF)

    def finish_rows():
        pl.when(has_right)(feats[0].wait_recv)
        pl.when(has_left)(feats[1].wait_recv)
        pre = mm_nt(embed_t[...], feat_rows[:, :inputs])
        gate = sigmoid(pre)
        silu = pre * gate
        latent[:, grid:] = silu.astype(BF)
        slope[:, grid:] = gate + silu * (1.0 - gate)

    def gradients():
        back[...] = (mm(wsend_t[...], total[...]) * slope[...]).astype(BF)

    def partial(lo, hi):
        return mm_nt(back[:, :grid], feat[lo:hi, :]) + mm(back[:, grid:], feat_rows[:, lo:hi])

    def sender_part():
        return mm_nt(total[...], latent[...])

    def receiver_sums(rows):
        sums = mm_nt(pairs[0, rows, :], hot_recv[0])
        for step in range(1, steps):
            sums += mm_nt(pairs[step, rows, :], hot_recv[step])
        return sums.astype(BF)

    def receiver_part():
        return mm(receiver_sums(slice(width, 2 * width)), nodes[...])

    part_copies = [
        remote(part_out.at[at], part_in.at[at], part_send.at[at], part_recv.at[at], mate, chan)
        for at in range(len(cuts))
    ]
    sides = ((sender_part, send_out), (receiver_part, recv_out))
    e_copies = [
        remote(e_out.at[at], e_in.at[at], e_send.at[at], e_recv.at[at], mate, chan) for at in range(2)
    ]
    ef_copies = [
        remote(e_final.at[at], e_final.at[at], ef_send.at[at], ef_recv.at[at], mate, chan) for at in range(2)
    ]
    final_copies = [
        remote(final.at[at], final.at[at], final_send.at[at], final_recv.at[at], mate, chan)
        for at in range(len(cuts))
    ]

    @pl.when(core == 0)
    def _():
        finish_rows()
        gradients()
        for at, (lo, hi) in enumerate(cuts):
            if hi - lo < LANES:
                part_out[at] = jnp.zeros_like(part_out[at])
            part_out[at, :, : hi - lo] = partial(lo, hi).astype(BF)
            part_copies[at].start()
        copies = []
        for side, (own_part, _) in enumerate(sides):
            value = own_part()
            e_copies[side].wait_recv()
            e_planes[side, chip] = (value + e_in[side].astype(F32)).astype(BF)
            copies.append([])
            for at, peer in enumerate(peers):
                copy = remote(
                    e_planes.at[side, chip], e_planes.at[side, chip], ep_send.at[side, at], ep_recv.at[side, chip],
                    peer, chan,
                )
                copy.start()
                copies[side].append(copy)
        mesh_out[...] = receiver_sums(slice(0, width))
        for side, (_, out) in enumerate(sides):
            for at, peer in enumerate(peers):
                slot = lax.div(peer, 2)
                remote(
                    e_planes.at[side, slot], e_planes.at[side, slot], ep_send.at[side, at], ep_recv.at[side, slot],
                    peer, chan,
                ).wait_recv()
            value = e_planes[side, 0].astype(F32)
            for at in range(1, chips):
                value += e_planes[side, at].astype(F32)
            e_final[side] = value
            ef_copies[side].start()
            out[...] = value
        for at, (lo, hi) in enumerate(cuts):
            final_copies[at].wait_recv()
            late_out[:, lo:hi] = final[at, :, : hi - lo]
        for copy in part_copies + sum(copies, []) + ef_copies:
            copy.wait_send()

    @pl.when(core == 1)
    def _():
        mine = pl.ds(pl.multiple_of(chan * width, width), width)
        first = pl.ds(pl.multiple_of(ordered[0] * width, width), width)
        finish_rows()
        e_out[0] = sender_part().astype(BF)
        e_copies[0].start()
        gradients()
        for at, (lo, hi) in enumerate(cuts):
            part_own[at, :, : hi - lo] = partial(lo, hi)
        e_out[1] = receiver_part().astype(BF)
        e_copies[1].start()
        moves = []
        for at, (lo, hi) in enumerate(cuts):
            part_copies[at].wait_recv()
            if hi - lo < LANES:
                z_out[at] = jnp.zeros_like(z_out[at])
            wide = slice(0, hi - lo)
            z_out[at, :, wide] = (part_own[at, :, wide] + part_in[at, :, wide].astype(F32)).astype(BF)
            copy = remote(
                z_out.at[at, first], z_in.at[at, chan], z_send.at[at, 0], z_recv.at[at, chan], band, ordered[0]
            )
            copy.start()
            moves.append(copy)
        for step, peer in enumerate(ordered[1:], 1):
            block = pl.ds(pl.multiple_of(peer * width, width), width)
            for at in range(len(cuts)):
                copy = remote(
                    z_out.at[at, block], z_in.at[at, chan], z_send.at[at, step], z_recv.at[at, chan], band, peer
                )
                copy.start()
                moves.append(copy)
        mesh_out[...] = receiver_sums(slice(0, width))
        swaps = []
        for at, (lo, hi) in enumerate(cuts):
            value = z_out[at, mine, :].astype(F32)
            for step, peer in enumerate(ordered):
                remote(
                    z_out.at[at, mine], z_in.at[at, peer], z_send.at[at, step], z_recv.at[at, peer], band, peer
                ).wait_recv()
                value += z_in[at, peer].astype(F32)
            planes[at, chip] = value.astype(BF)
            swaps.append([])
            for step, peer in enumerate(peers):
                copy = remote(
                    planes.at[at, chip], planes.at[at, chip], plane_send.at[at, step], plane_recv.at[at, chip],
                    peer, chan,
                )
                copy.start()
                swaps[at].append(copy)
        for at, (lo, hi) in enumerate(cuts):
            for step, peer in enumerate(peers):
                slot = lax.div(peer, 2)
                remote(
                    planes.at[at, slot], planes.at[at, slot], plane_send.at[at, step], plane_recv.at[at, slot],
                    peer, chan,
                ).wait_recv()
            value = planes[at, 0].astype(F32)
            for other in range(1, chips):
                value += planes[at, other].astype(F32)
            final[at] = value
            final_copies[at].start()
        for side, (_, out) in enumerate(sides):
            ef_copies[side].wait_recv()
            out[...] = e_final[side]
        for at, (lo, hi) in enumerate(cuts):
            late_out[:, lo:hi] = final[at, :, : hi - lo]
        for copy in e_copies + final_copies + moves + sum(swaps, []):
            copy.wait_send()

    for has, at in ((has_left, 0), (has_right, 1)):
        pl.when(has)(rows[at].wait_send)
        pl.when(has)(feats[at].wait_send)


def place(count, *refs):
    sems = refs[2 * count]
    copies = [
        pltpu.make_async_copy(refs[at], refs[count + at], sems.at[at]) for at in range(count)
    ]
    for copy in copies:
        copy.start()
    for copy in copies:
        copy.wait()


def on_device(
    grid_feat, w_embed, w_send, w_recv, mesh_nodes, mesh_cot, send_index, edge_source, edge_receiver
):
    bands = lax.axis_size("band")
    chans = lax.axis_size("chan")
    chips = bands // 2
    grid, inputs = grid_feat.shape
    latents, width = w_send.shape
    mesh_count = mesh_nodes.shape[0]
    cap = send_index.shape[2]
    slots = grid + 2 * cap
    edges = edge_source.shape[0]
    chunk = math.gcd(edges, 2048)
    steps = edges // chunk
    cuts = -(-inputs // LANES)
    wide = cuts * LANES
    vmem = pl.BlockSpec(memory_space=pltpu.VMEM)
    arrays = (
        grid_feat.T, w_embed, w_send.T, w_recv.T, mesh_nodes, mesh_cot.T,
        send_index, edge_source, edge_receiver,
    )
    scratch = [
        ((latents, inputs), BF),
        ((latents, width), BF),
        ((latents, slots), BF),
        ((latents, slots), F32),
        ((latents, slots), BF),
        ((2 * cap, width), BF),
        ((2 * cap, width), BF),
        ((2 * cap, wide), BF),
        ((2 * cap, wide), BF),
        ((2 * width, slots + mesh_count), BF),
        ((steps, mesh_count, chunk), jnp.float8_e4m3fn),
        ((steps, slots, chunk), jnp.float8_e4m3fn),
        ((steps, 2 * width, chunk), F32),
        ((steps, 2 * width, chunk), BF),
        ((width, slots), F32),
        ((width, slots), BF),
        ((cuts, latents, LANES), F32),
        ((cuts, latents, LANES), BF),
        ((cuts, latents, LANES), BF),
        ((cuts, latents, LANES), BF),
        ((cuts, chans, width, LANES), BF),
        ((cuts, chips, width, LANES), BF),
        ((cuts, width, LANES), F32),
        ((2, width, latents), BF),
        ((2, width, latents), BF),
        ((2, chips, width, latents), BF),
        ((2, width, latents), F32),
    ]
    sems = [
        (2,), (2,), (2,), (2,), (cuts,), (cuts,), (cuts, chans - 1), (cuts, chans),
        (cuts, chips - 1), (cuts, chips), (cuts,), (cuts,), (2,), (2,), (2, chips - 1), (2, chips), (2,), (2,),
    ]
    outs = pl.pallas_call(
        functools.partial(body, bands, chans, chunk),
        out_shape=(
            pltpu.VMEM((width, mesh_count), BF),
            pltpu.VMEM((width, inputs), F32),
            pltpu.VMEM((width, latents), F32),
            pltpu.VMEM((width, latents), F32),
        ),
        in_specs=[pl.BlockSpec(memory_space=pl.ANY)] * 9,
        out_specs=(vmem,) * 4,
        scratch_shapes=[pltpu.VMEM(array.shape, array.dtype) for array in arrays]
        + [pltpu.SemaphoreType.DMA((9,))]
        + [pltpu.VMEM(shape, kind) for shape, kind in scratch]
        + [pltpu.SemaphoreType.DMA(shape) for shape in sems],
        compiler_params=pltpu.CompilerParams(collective_id=0, has_side_effects=True),
    )(*arrays)
    anywhere = pl.BlockSpec(memory_space=pl.ANY)
    placed = pl.pallas_call(
        functools.partial(place, len(outs)),
        out_shape=tuple(jax.ShapeDtypeStruct(out.shape, out.dtype) for out in outs),
        in_specs=[vmem] * len(outs),
        out_specs=(anywhere,) * len(outs),
        scratch_shapes=[pltpu.SemaphoreType.DMA((len(outs),))],
    )(*(pltpu.with_memory_space_constraint(out, pltpu.VMEM) for out in outs))
    return tuple(out.T for out in placed)


def solution(mesh):
    placed = (
        P("band", None),
        P(),
        P(None, "chan"),
        P(None, "chan"),
        P("band", None),
        P("band", "chan"),
        P("band", None, None),
        P("band"),
        P("band"),
    )
    return jax.shard_map(
        on_device,
        mesh=mesh,
        in_specs=placed,
        out_specs=(P("band", "chan"), P(None, "chan"), P(None, "chan"), P(None, "chan")),
        check_vma=False,
    )
```
